32 devices in a mesh: seq: 8 (over z, y), tp: 4 (over x, core).
Axes of the slice: x: 2, y: 2, z: 4, core: 2. Of those that a mesh axis runs over, the one named last changes fastest.
Arguments:
- tokens: bfloat16 [6144, 4096], P('seq'), may hold values from -6 to 6
- query_weight: bfloat16 [4096, 2048], P('seq', 'tp'), may hold values from -0.09375 to 0.09375
- key_weight: bfloat16 [4096, 2048], P('seq', 'tp'), may hold values from -0.09375 to 0.09375
- value_weight: bfloat16 [4096, 2048], P('seq', 'tp'), may hold values from -0.09375 to 0.09375
- gate_weight: bfloat16 [4096, 16], P('seq', 'tp'), may hold values from -0.09375 to 0.09375
- decay_rate: float32 [16], P('tp'), may hold values from 3.2552085e-05 to 0.04
- norm_gain: float32 [2048], P('tp'), may hold values from 0.5 to 1.5
- out_weight: bfloat16 [2048, 4096], P(None, 'tp'), may hold values from -0.125 to 0.125
Outputs:
- mixed: bfloat16 [6144, 4096], P('seq', 'tp')
The draws below stay inside these ranges and needn't reach their ends.
All inputs are finite; a program needn't handle non-finite values.
Results may differ from the reference program's by a relative error of at most 0.006.
The reference program's roundings to bfloat16 on the way count: a program that leaves them out, or rounds other values in their place, can miss the bound.
Values may be sent and summed in bfloat16 or wider, within the bound.
A program may use at most 128 MiB of HBM per device.

```python
import math
import jax
import jax.numpy as jnp
from jax import lax

D = 4096
H = 16
K = 128
TOK_DEV = 768
TOKENS = 6144


def level_of(own_key, shape, shards, smallest, high):
    def one(dim, blocks):
        steps = jax.random.uniform(jax.random.fold_in(jax.random.fold_in(own_key, 6), dim), (blocks,), jnp.float32, smallest / len(shards), high / len(shards))
        return jnp.repeat(jnp.exp(steps), shape[dim] // blocks).reshape((-1,) + (1,) * (len(shape) - dim - 1))

    level = one(*shards[0])
    for cut in shards[1:]:
        level = level * one(*cut)
    return level


def centred(own_key, dims, spread, reach, pieces=(), kind=jnp.bfloat16):
    loudness = level_of(own_key, dims, pieces, -0.22, 0.18) if pieces else 1.0
    values = jax.random.normal(own_key, dims, jnp.float32) * spread * loudness
    return jnp.minimum(jnp.maximum(values, -reach), reach).astype(kind)


def setup_inputs(seed: int = 0) -> dict:
    key_of = jax.random.split(jax.random.key(seed), 9)
    return {
        "tokens": centred(key_of[0], (TOKENS, D), 1.0, 6.0, ((0, 8),)),
        "query_weight": centred(key_of[1], (D, H * K), D ** -0.5, 0.09375, ((0, 8), (1, 4))),
        "key_weight": centred(key_of[2], (D, H * K), D ** -0.5, 0.09375, ((0, 8), (1, 4))),
        "value_weight": centred(key_of[3], (D, H * K), D ** -0.5, 0.09375, ((0, 8), (1, 4))),
        "gate_weight": centred(key_of[4], (D, H), D ** -0.5, 0.09375, ((0, 8), (1, 4))),
        "decay_rate": jnp.clip(jnp.exp(math.log(0.04) - 7.1137933 * jax.random.uniform(key_of[5], (H,), jnp.float32) ** level_of(key_of[5], (H,), ((0, 4),), -0.2, 0.2)), 3.255208503105678e-05, 0.04),
        "norm_gain": jnp.clip(1.0 + 0.1 * jax.random.normal(key_of[6], (H * K,), jnp.float32), 0.5, 1.5),
        "out_weight": centred(key_of[7], (H * K, D), (H * K) ** -0.5, 0.125, ((1, 4),)),
    }


def reference(tokens, query_weight, key_weight, value_weight, gate_weight, decay_rate, norm_gain, out_weight):
    query_proj = jnp.dot(tokens, query_weight, preferred_element_type=jnp.float32).astype(jnp.bfloat16)
    key_proj = jnp.dot(tokens, key_weight, preferred_element_type=jnp.float32).astype(jnp.bfloat16)
    value_proj = jnp.dot(tokens, value_weight, preferred_element_type=jnp.float32).astype(jnp.bfloat16)
    gate_logit = jnp.dot(tokens, gate_weight, preferred_element_type=jnp.float32)
    log_decay = -decay_rate[None, :] * jax.nn.softplus(gate_logit)
    block_count = TOKENS // TOK_DEV
    query_blocks = query_proj.reshape(block_count, TOK_DEV, H, K)
    key_blocks = key_proj.reshape(block_count, TOK_DEV, H, K)
    value_blocks = value_proj.reshape(block_count, TOK_DEV, H, K)
    decay_blocks = log_decay.reshape(block_count, TOK_DEV, H)
    causal = jnp.tril(jnp.ones((TOK_DEV, TOK_DEV), dtype=bool))[None, :, :]

    def block_step(prev_state, items):
        query_blk, key_blk, value_blk, decay_blk = items
        within = jnp.cumsum(decay_blk, axis=0)
        block_total = within[-1]
        query_wide = query_blk.astype(jnp.float32)
        key_wide = key_blk.astype(jnp.float32)
        value_full_width = value_blk.astype(jnp.float32)
        query_scaled = (jnp.exp(within)[:, :, None] * query_wide).astype(jnp.bfloat16)
        state_bfloat = prev_state.astype(jnp.bfloat16)
        carried_state = jnp.einsum('fys,ysu->fyu', query_scaled.astype(jnp.float32), state_bfloat.astype(jnp.float32))
        scores = jnp.einsum('thk,shk->hts', query_wide, key_wide)
        decay_gap = within.T[:, :, None] - within.T[:, None, :]
        attn = jnp.where(causal, scores * jnp.exp(jnp.where(causal, decay_gap, 0.0)), 0.0).astype(jnp.bfloat16)
        local_part = jnp.einsum('hts,shv->thv', attn.astype(jnp.float32), value_full_width)
        key_scaled = (jnp.exp(block_total[None, :] - within)[:, :, None] * key_wide).astype(jnp.bfloat16)
        shard_local_state = jnp.einsum('gfw,gfz->fwz', key_scaled.astype(jnp.float32), value_full_width)
        next_state = jnp.exp(block_total)[:, None, None] * prev_state + shard_local_state
        return (next_state, carried_state + local_part)
    start_state = jnp.zeros((H, K, K), jnp.float32)
    _, head_out = lax.scan(block_step, start_state, (query_blocks, key_blocks, value_blocks, decay_blocks))
    mean_square = lax.optimization_barrier(jnp.mean(head_out * head_out, axis=-1, keepdims=True))
    normed = (head_out * lax.rsqrt(mean_square + 1e-05)).reshape(TOKENS, H * K) * norm_gain[None, :]
    normed = normed.astype(jnp.bfloat16)
    return jnp.dot(normed, out_weight, preferred_element_type=jnp.float32).astype(jnp.bfloat16)
```

```python
import functools

import jax
import jax.numpy as jnp
from jax import lax
from jax.experimental import pallas as pl
from jax.experimental.pallas import tpu as pltpu
from jax.sharding import PartitionSpec as P

HALVES = 2
MESH = pl.DeviceIdType.MESH


def project_kernel(seq, wide, *refs):
    tok_ref, gate_in, key_in, value_in, query_in = refs[:5]
    gate_out, key_out, value_out, query_out = refs[5:9]
    gate_buf, kvq_buf, gate_acc, acc, own_sem, send_own, send_line, send_peer, recv_sem = refs[9:]
    rows = key_in.shape[0]
    half = key_in.shape[1] // HALVES
    cross = 2
    line = seq // cross
    me = lax.axis_index("seq")
    a, b = me // cross, me % cross
    peer = a * cross + (1 - b)

    def buffer(piece, source):
        if piece == 0:
            return gate_buf.at[source]
        return kvq_buf.at[piece - 1, source]

    def tok(source):
        if wide:
            return tok_ref[:, pl.ds(pl.multiple_of(source * rows, rows), rows)]
        return tok_ref[source]

    def copy(piece, source, sem, target):
        return pltpu.make_async_remote_copy(
            src_ref=buffer(piece, source),
            dst_ref=buffer(piece, source),
            send_sem=sem,
            recv_sem=recv_sem.at[piece, source],
            device_id={"seq": target},
            device_id_type=MESH,
        )

    def arrive(piece, source):
        copy(piece, source, send_own.at[piece, 0], peer).wait_recv()

    phases = [[1, 0, 2, 3], [4, 5, 6]]
    peer_first = (1,)

    loads = [pltpu.make_async_copy(gate_in, gate_buf.at[me], own_sem.at[0])]
    for index in range(3 * HALVES):
        source_ref = (key_in, value_in, query_in)[index % 3]
        at = (index // 3) * half
        loads.append(
            pltpu.make_async_copy(
                source_ref.at[:, pl.ds(at, half)], kvq_buf.at[index, me], own_sem.at[index + 1]
            )
        )
    for load in loads:
        load.start()

    barrier = pltpu.get_barrier_semaphore()
    has_up, has_down = a < line - 1, a > 0
    pl.semaphore_signal(barrier, inc=1, device_id={"seq": peer}, device_id_type=MESH)

    @pl.when(has_up)
    def _():
        pl.semaphore_signal(barrier, inc=1, device_id={"seq": me + cross}, device_id_type=MESH)

    @pl.when(has_down)
    def _():
        pl.semaphore_signal(barrier, inc=1, device_id={"seq": me - cross}, device_id_type=MESH)

    pl.semaphore_wait(barrier, 1 + has_up.astype(jnp.int32) + has_down.astype(jnp.int32))

    def send_mine(pieces):
        for piece in pieces:
            loads[piece].wait()
            copy(piece, me, send_own.at[piece, 0], peer).start()

            @pl.when(has_up)
            def _():
                copy(piece, me, send_own.at[piece, 1], me + cross).start()

            @pl.when(has_down)
            def _():
                copy(piece, me, send_own.at[piece, 2], me - cross).start()

    def multiply(piece, source):
        x = tok(source)
        if piece == 0:
            gate_acc[...] += lax.dot_general(
                x, gate_buf[source], (((1,), (1,)), ((), ())), preferred_element_type=jnp.float32
            )
        else:
            acc[piece - 1] += jnp.dot(
                x, kvq_buf[piece - 1, source], preferred_element_type=jnp.float32
            )

    def step_of(t):
        d = 1 + t // 2
        sign = 1 - 2 * (t % 2)
        origin = a - sign * d
        ahead = a + sign
        valid = (origin >= 0) & (origin < line)
        onward = valid & (ahead >= 0) & (ahead < line)
        return origin, valid, onward, me + sign * cross

    def from_peer(pieces, t):
        origin, valid, _, _ = step_of(t)

        @pl.when(valid)
        def _():
            source = origin * cross + (1 - b)
            for piece in pieces:
                if piece not in peer_first:
                    arrive(piece, source)
                multiply(piece, source)

    gate_acc[...] = jnp.zeros_like(gate_acc)
    acc[...] = jnp.zeros_like(acc)
    steps = 2 * (line - 1)
    for number, pieces in enumerate(phases):
        if number == 0:
            send_mine(pieces)
        for piece in pieces:
            if piece in peer_first:
                arrive(piece, peer)

                @pl.when(has_up)
                def _():
                    copy(piece, peer, send_line.at[piece, peer], me + cross).start()

                @pl.when(has_down)
                def _():
                    copy(piece, peer, send_peer.at[piece, peer], me - cross).start()

        for piece in pieces:
            multiply(piece, me)

        @pl.loop(0, steps)
        def _(t):
            origin, valid, onward, target = step_of(t)
            source = origin * cross + b
            other = origin * cross + (1 - b)

            @pl.when(valid)
            def _():
                for piece in pieces:
                    arrive(piece, source)

                    @pl.when(onward)
                    def _():
                        copy(piece, source, send_line.at[piece, source], target).start()

                    if piece in peer_first:
                        arrive(piece, other)

                        @pl.when(onward)
                        def _():
                            copy(piece, other, send_line.at[piece, other], target).start()
                    else:
                        copy(piece, source, send_peer.at[piece, source], peer).start()
                for piece in pieces:
                    multiply(piece, source)

            @pl.when(t == 1)
            def _():
                for piece in pieces:
                    if piece not in peer_first:
                        arrive(piece, peer)
                    multiply(piece, peer)

            @pl.when(t >= 2)
            def _():
                from_peer(pieces, t - 2)

        if number + 1 < len(phases):
            send_mine(phases[number + 1])

        @pl.loop(steps - 2, steps)
        def _(t):
            from_peer(pieces, t)

    gate_out[...] = gate_acc[...]
    for index in range(3 * HALVES):
        out = (key_out, value_out, query_out)[index % 3]
        at = (index // 3) * half
        out[:, pl.ds(at, half)] = acc[index].astype(jnp.bfloat16)

    for pieces in phases:
        for piece in pieces:
            copy(piece, me, send_own.at[piece, 0], peer).wait_send()

            @pl.when(has_up)
            def _():
                copy(piece, me, send_own.at[piece, 1], peer).wait_send()

            @pl.when(has_down)
            def _():
                copy(piece, me, send_own.at[piece, 2], peer).wait_send()

            if piece in peer_first:

                @pl.when(has_up)
                def _():
                    copy(piece, peer, send_line.at[piece, peer], peer).wait_send()

                @pl.when(has_down)
                def _():
                    copy(piece, peer, send_peer.at[piece, peer], peer).wait_send()

        @pl.loop(0, steps)
        def _(t):
            origin, valid, onward, target = step_of(t)
            source = origin * cross + b
            other = origin * cross + (1 - b)
            for piece in pieces:

                @pl.when(onward)
                def _():
                    copy(piece, source, send_line.at[piece, source], peer).wait_send()
                    if piece in peer_first:
                        copy(piece, other, send_line.at[piece, other], peer).wait_send()

                if piece not in peer_first:

                    @pl.when(valid)
                    def _():
                        copy(piece, source, send_peer.at[piece, source], peer).wait_send()


def project(seq, tokens, query_weight, key_weight, value_weight, gate_weight):
    count = tokens.shape[0]
    rows, width = query_weight.shape
    heads = gate_weight.shape[1]
    wide = rows % 128 == 0
    tok = tokens if wide else tokens.reshape(count, seq, rows).transpose(1, 0, 2)
    gate_t = jnp.pad(gate_weight.T, ((0, 16 - heads), (0, 0)))
    vmem = pl.BlockSpec(memory_space=pltpu.VMEM)
    hbm = pl.BlockSpec(memory_space=pl.ANY)
    pieces = 3 * HALVES + 1
    wide_out = jax.ShapeDtypeStruct((count, width), jnp.bfloat16)
    dma = pltpu.SemaphoreType.DMA
    return pl.pallas_call(
        functools.partial(project_kernel, seq, wide),
        out_shape=(jax.ShapeDtypeStruct((count, 16), jnp.float32), wide_out, wide_out, wide_out),
        in_specs=[vmem, hbm, hbm, hbm, hbm],
        out_specs=(vmem, vmem, vmem, vmem),
        scratch_shapes=[
            pltpu.VMEM((seq, 16, rows), jnp.bfloat16),
            pltpu.VMEM((3 * HALVES, seq, rows, width // HALVES), jnp.bfloat16),
            pltpu.VMEM((count, 16), jnp.float32),
            pltpu.VMEM((3 * HALVES, count, width // HALVES), jnp.float32),
            dma((pieces,)),
            dma((pieces, 3)),
            dma((pieces, seq)),
            dma((pieces, seq)),
            dma((pieces, seq)),
        ],
        compiler_params=pltpu.CompilerParams(
            collective_id=0, has_side_effects=True, vmem_limit_bytes=60 * 1024 * 1024
        ),
    )(tok, gate_t, key_weight, value_weight, query_weight)


def on_device(
    seq, tokens, query_weight, key_weight, value_weight, gate_weight, decay_rate, norm_gain, out_weight
):
    tok_rows = tokens.shape[0]
    head_count = decay_rate.shape[0]
    proj_width = query_weight.shape[1]
    head_size = proj_width // head_count
    gate_wide, key_proj, value_proj, query_proj = project(
        seq, tokens, query_weight, key_weight, value_weight, gate_weight
    )
    gate_logit = gate_wide[:, :head_count]
    query_heads = query_proj.reshape(tok_rows, head_count, head_size)
    key_heads = key_proj.reshape(tok_rows, head_count, head_size)
    value_per_head = value_proj.reshape(tok_rows, head_count, head_size)
    log_decay = -decay_rate[None, :] * jax.nn.softplus(gate_logit)
    within = jnp.cumsum(log_decay, axis=0)
    block_total = within[-1]
    key_scaled = (jnp.exp(block_total[None, :] - within)[:, :, None] * key_heads).astype(
        jnp.bfloat16
    )
    shard_local_state = jnp.einsum(
        "gfw,gfz->fwz", key_scaled, value_per_head, preferred_element_type=jnp.float32
    )
    all_totals = lax.all_gather(block_total[None, :], "seq", axis=0, tiled=True)
    running_sum = jnp.cumsum(all_totals, axis=0)
    seq_rank = lax.axis_index("seq")
    before = lax.dynamic_index_in_dim(running_sum, jnp.maximum(seq_rank - 1, 0), 0, keepdims=False)
    piece = lax.all_gather(shard_local_state[None], "seq", axis=0, tiled=True)
    piece_rows = piece.shape[0]
    positions = jnp.arange(piece_rows, dtype=jnp.int32)
    earlier_ok = (positions < seq_rank)[:, None]
    factor = jnp.where(
        earlier_ok, jnp.exp(jnp.where(earlier_ok, before[None, :] - running_sum, 0.0)), 0.0
    )
    prefix_state = jnp.sum(factor[:, :, None, None] * piece, axis=0)
    query_scaled = (jnp.exp(within)[:, :, None] * query_heads).astype(jnp.bfloat16)
    carried_state = jnp.einsum(
        "fys,ysu->fyu",
        query_scaled,
        prefix_state.astype(jnp.bfloat16),
        preferred_element_type=jnp.float32,
    )
    scores = jnp.einsum("thk,shk->hts", query_heads, key_heads, preferred_element_type=jnp.float32)
    row_index = lax.broadcasted_iota(jnp.int32, (tok_rows, tok_rows), 0)
    col_index = lax.broadcasted_iota(jnp.int32, (tok_rows, tok_rows), 1)
    causal = (col_index <= row_index)[None, :, :]
    decay_gap = within.T[:, :, None] - within.T[:, None, :]
    attn = jnp.where(causal, scores * jnp.exp(jnp.where(causal, decay_gap, 0.0)), 0.0).astype(
        jnp.bfloat16
    )
    local_part = jnp.einsum(
        "hts,shv->thv", attn, value_per_head, preferred_element_type=jnp.float32
    )
    head_out = carried_state + local_part
    mean_square = jnp.mean(head_out * head_out, axis=-1, keepdims=True)
    normed = (head_out * lax.rsqrt(mean_square + 1e-05)).reshape(tok_rows, proj_width) * norm_gain[
        None, :
    ]
    normed = normed.astype(jnp.bfloat16)
    mixed = jnp.dot(
        lax.all_gather(normed, "tp", axis=1, tiled=True),
        out_weight,
        preferred_element_type=jnp.float32,
    )
    return mixed.astype(jnp.bfloat16)


def solution(mesh):
    return jax.shard_map(
        functools.partial(on_device, mesh.shape["seq"]),
        mesh=mesh,
        in_specs=(
            P("seq", None),
            P("seq", "tp"),
            P("seq", "tp"),
            P("seq", "tp"),
            P("seq", "tp"),
            P("tp"),
            P("tp"),
            P(None, "tp"),
        ),
        out_specs=P("seq", "tp"),
        check_vma=False,
    )
```

```python
import functools

import jax
import jax.numpy as jnp
from jax import lax
from jax.experimental import pallas as pl
from jax.experimental.pallas import tpu as pltpu
from jax.sharding import PartitionSpec as P

HALVES = 2
MESH = pl.DeviceIdType.MESH


def layer_kernel(seq, tp, heads, wide, *refs):
    tok_ref, rate_ref, gain_ref, gate_in, key_in, value_in, query_in, out_in = refs[:8]
    mixed_ref = refs[8]
    gate_buf, kvq_buf, gate_acc, acc, out_buf, out_acc, wcol, wrow = refs[9:17]
    state_mine, state_peer, state_in, state_next, normed_buf = refs[17:22]
    own_sem, send_own, send_line, send_peer, recv_sem = refs[22:27]
    state_send, state_recv, normed_send, normed_recv = refs[27:31]
    rows = key_in.shape[0]
    half = key_in.shape[1] // HALVES
    cross = 2
    line = seq // cross
    me = lax.axis_index("seq")
    a, b = me // cross, me % cross
    peer = a * cross + (1 - b)
    count = acc.shape[1]
    head_size = 2 * half // heads
    per_half = heads // HALVES
    block = 256 if count % 256 == 0 else count
    blocks = count // block
    col = lax.axis_index("tp")
    pair_col = col + 1 - 2 * (col % 2)
    groups = tp // 2

    def buffer(piece, source):
        if piece == 0:
            return gate_buf.at[source]
        return kvq_buf.at[piece - 1, source]

    def tok(source):
        if wide:
            return tok_ref[:, pl.ds(pl.multiple_of(source * rows, rows), rows)]
        return tok_ref[source]

    def copy(piece, source, sem, target):
        return pltpu.make_async_remote_copy(
            src_ref=buffer(piece, source),
            dst_ref=buffer(piece, source),
            send_sem=sem,
            recv_sem=recv_sem.at[piece, source],
            device_id={"seq": target},
            device_id_type=MESH,
        )

    def arrive(piece, source):
        copy(piece, source, send_own.at[piece, 0], peer).wait_recv()

    phases = [[1, 0, 2, 3], [4, 5], [6]]
    peer_first = (1,)

    loads = [pltpu.make_async_copy(gate_in, gate_buf.at[me], own_sem.at[0])]
    for index in range(3 * HALVES):
        source_ref = (key_in, value_in, query_in)[index % 3]
        at = (index // 3) * half
        loads.append(
            pltpu.make_async_copy(
                source_ref.at[:, pl.ds(at, half)], kvq_buf.at[index, me], own_sem.at[index + 1]
            )
        )
    for load in loads:
        load.start()
    out_load = pltpu.make_async_copy(out_in, out_buf, own_sem.at[3 * HALVES + 1])
    out_load.start()

    barrier = pltpu.get_barrier_semaphore()
    has_up, has_down = a < line - 1, a > 0
    pl.semaphore_signal(barrier, inc=1, device_id={"seq": peer}, device_id_type=MESH)

    @pl.when(has_up)
    def _():
        pl.semaphore_signal(barrier, inc=1, device_id={"seq": me + cross}, device_id_type=MESH)

    @pl.when(has_down)
    def _():
        pl.semaphore_signal(barrier, inc=1, device_id={"seq": me - cross}, device_id_type=MESH)

    pl.semaphore_signal(barrier, inc=1, device_id={"tp": pair_col}, device_id_type=MESH)
    for g in range(1, groups):
        pl.semaphore_signal(
            barrier, inc=1, device_id={"tp": lax.rem(col + 2 * g, tp)}, device_id_type=MESH
        )
    pl.semaphore_wait(barrier, 1 + groups + has_up.astype(jnp.int32) + has_down.astype(jnp.int32))

    def send_mine(pieces):
        for piece in pieces:
            loads[piece].wait()
            copy(piece, me, send_own.at[piece, 0], peer).start()

            @pl.when(has_up)
            def _():
                copy(piece, me, send_own.at[piece, 1], me + cross).start()

            @pl.when(has_down)
            def _():
                copy(piece, me, send_own.at[piece, 2], me - cross).start()

    def multiply(piece, source):
        x = tok(source)
        if piece == 0:
            gate_acc[...] += lax.dot_general(
                x, gate_buf[source], (((1,), (1,)), ((), ())), preferred_element_type=jnp.float32
            )
        else:
            acc[piece - 1] += jnp.dot(
                x, kvq_buf[piece - 1, source], preferred_element_type=jnp.float32
            )

    def step_of(t):
        d = 1 + t // 2
        sign = 1 - 2 * (t % 2)
        origin = a - sign * d
        ahead = a + sign
        valid = (origin >= 0) & (origin < line)
        onward = valid & (ahead >= 0) & (ahead < line)
        return origin, valid, onward, me + sign * cross

    def from_peer(pieces, t):
        origin, valid, _, _ = step_of(t)

        @pl.when(valid)
        def _():
            source = origin * cross + (1 - b)
            for piece in pieces:
                if piece not in peer_first:
                    arrive(piece, source)
                multiply(piece, source)

    lo_state = per_half * head_size

    def decays():
        logits = jnp.concatenate(
            [gate_acc[...], jnp.zeros((count, 128 - gate_acc.shape[1]), jnp.float32)], axis=1
        ).T[:8]
        soft = jnp.maximum(logits, 0.0) + jnp.log1p(jnp.exp(-jnp.abs(logits)))
        total = -rate_ref[...] * soft
        lane = lax.broadcasted_iota(jnp.int32, total.shape, 1)
        reach = 1
        while reach < count:
            total = total + jnp.where(lane >= reach, pltpu.roll(total, reach, 1), 0.0)
            reach *= 2
        wrow[...] = total
        wcol[...] = jnp.concatenate(
            [total, jnp.zeros((120, count), jnp.float32)], axis=0
        ).T

    def state_copy(ref_from, ref_to, h, send, recv, target):
        return pltpu.make_async_remote_copy(
            src_ref=ref_from.at[h],
            dst_ref=ref_to.at[h],
            send_sem=state_send.at[send, h],
            recv_sem=state_recv.at[recv, h],
            device_id={"seq": target},
            device_id_type=MESH,
        )

    def pair_state(h):
        return state_copy(state_mine, state_peer, h, 0, 0, peer)

    def line_state(h):
        return state_copy(state_next, state_in, h, 1, 1, me + cross)

    def back_state(h):
        return state_copy(state_in, state_in, h, 2, 1, peer)

    def local_state(h):
        for j in range(per_half):
            head = h * per_half + j
            cols = slice(j * head_size, (j + 1) * head_size)
            within = wcol[:, head : head + 1]
            last = wcol[count - 1 : count, head : head + 1]
            key = acc[3 * h, :, cols].astype(jnp.bfloat16).astype(jnp.float32)
            scaled = (jnp.exp(last - within) * key).astype(jnp.bfloat16)
            value = acc[3 * h + 1, :, cols].astype(jnp.bfloat16)
            state_mine[h, j * head_size : (j + 1) * head_size] = lax.dot_general(
                scaled, value, (((0,), (0,)), ((), ())), preferred_element_type=jnp.float32
            )
            state_mine[h, lo_state + j : lo_state + j + 1] = jnp.broadcast_to(last, (1, head_size))

        @pl.when(b == 0)
        def _():
            pair_state(h).start()

        @pl.when(a == 0)
        def _():
            state_in[h] = jnp.zeros(state_in.shape[1:], jnp.float32)

    def chain(h):
        @pl.when(b == 1)
        def _():
            pair_state(h).wait_recv()

            @pl.when(has_down)
            def _():
                line_state(h).wait_recv()
                back_state(h).start()

            for j in range(per_half):
                at = slice(j * head_size, (j + 1) * head_size)
                tot = slice(lo_state + j, lo_state + j + 1)
                before = jnp.exp(state_peer[h, tot]) * state_in[h, at] + state_peer[h, at]
                state_peer[h, at] = before
                state_next[h, at] = jnp.exp(state_mine[h, tot]) * before + state_mine[h, at]

            @pl.when(has_up)
            def _():
                line_state(h).start()

    def chain_end(h):
        @pl.when(b == 0)
        def _():
            @pl.when(has_down)
            def _():
                back_state(h).wait_recv()

            state_peer[h, :lo_state] = state_in[h]

    def normed_copy(h, i, source, send, target):
        at = pl.ds(i * block, block)
        return pltpu.make_async_remote_copy(
            src_ref=normed_buf.at[h, source, at],
            dst_ref=normed_buf.at[h, source, at],
            send_sem=normed_send.at[h, i, send],
            recv_sem=normed_recv.at[h, i, source],
            device_id={"tp": target},
            device_id_type=MESH,
        )

    def far(g):
        return lax.rem(col + 2 * g, tp)

    def far_pair(g):
        return lax.rem(pair_col + 2 * g, tp)

    def attention(h):
        for i in range(blocks):
            t_at = slice(i * block, (i + 1) * block)
            upto = (i + 1) * block
            row = i * block + lax.broadcasted_iota(jnp.int32, (block, upto), 0)
            causal = lax.broadcasted_iota(jnp.int32, (block, upto), 1) <= row
            for j in range(per_half):
                head = h * per_half + j
                cols = slice(j * head_size, (j + 1) * head_size)
                query = acc[3 * h + 2, t_at, cols].astype(jnp.bfloat16)
                key = acc[3 * h, :upto, cols].astype(jnp.bfloat16)
                value = acc[3 * h + 1, :upto, cols].astype(jnp.bfloat16)
                within = wcol[t_at, head : head + 1]
                scores = lax.dot_general(
                    query, key, (((1,), (1,)), ((), ())), preferred_element_type=jnp.float32
                )
                gap = within - wrow[head : head + 1, :upto]
                attn = jnp.where(causal, scores * jnp.exp(jnp.where(causal, gap, 0.0)), 0.0)
                local = jnp.dot(
                    attn.astype(jnp.bfloat16), value, preferred_element_type=jnp.float32
                )
                scaled = (jnp.exp(within) * query.astype(jnp.float32)).astype(jnp.bfloat16)
                state = state_peer[h, j * head_size : (j + 1) * head_size].astype(jnp.bfloat16)
                head_out = local + jnp.dot(scaled, state, preferred_element_type=jnp.float32)
                square = jnp.mean(head_out * head_out, axis=-1, keepdims=True)
                gain = gain_ref[:, head * head_size : (head + 1) * head_size]
                normed_buf[h, col, t_at, cols] = (
                    head_out * lax.rsqrt(square + 1e-05) * gain
                ).astype(jnp.bfloat16)
            for g in range(1, groups):
                normed_copy(h, i, col, g, far(g)).start()
            normed_copy(h, i, col, 0, pair_col).start()

    def relay(h, i):
        for g in range(1, groups):
            normed_copy(h, i, far(g), 0, pair_col).wait_recv()
            normed_copy(h, i, far(g), groups - 1 + g, pair_col).start()

    def mix(h, i, source):
        at = pl.ds(i * block, block)
        depth = pl.ds(pl.multiple_of((source * HALVES + h) * half, half), half)
        return jnp.dot(
            normed_buf[h, source, at], out_buf[depth, :], preferred_element_type=jnp.float32
        )

    def settle(h, i):
        at = pl.ds(i * block, block)
        total = mix(h, i, col)
        normed_copy(h, i, pair_col, 0, pair_col).wait_recv()
        total = total + mix(h, i, pair_col)
        for g in range(1, groups):
            total = total + mix(h, i, far(g))
            normed_copy(h, i, far_pair(g), 0, pair_col).wait_recv()
            total = total + mix(h, i, far_pair(g))
        if h == 0:
            out_acc[at, :] = total
        else:
            mixed_ref[at, :] = (out_acc[at, :] + total).astype(jnp.bfloat16)

    gate_acc[...] = jnp.zeros_like(gate_acc)
    acc[...] = jnp.zeros_like(acc)
    steps = 2 * (line - 1)
    for number, pieces in enumerate(phases):
        if number == 0:
            send_mine(pieces)
        for piece in pieces:
            if piece in peer_first:
                arrive(piece, peer)

                @pl.when(has_up)
                def _():
                    copy(piece, peer, send_line.at[piece, peer], me + cross).start()

                @pl.when(has_down)
                def _():
                    copy(piece, peer, send_peer.at[piece, peer], me - cross).start()

        for piece in pieces:
            multiply(piece, me)

        @pl.loop(0, steps)
        def _(t):
            origin, valid, onward, target = step_of(t)
            source = origin * cross + b
            other = origin * cross + (1 - b)

            @pl.when(valid)
            def _():
                for piece in pieces:
                    arrive(piece, source)

                    @pl.when(onward)
                    def _():
                        copy(piece, source, send_line.at[piece, source], target).start()

                    if piece in peer_first:
                        arrive(piece, other)

                        @pl.when(onward)
                        def _():
                            copy(piece, other, send_line.at[piece, other], target).start()
                    else:
                        copy(piece, source, send_peer.at[piece, source], peer).start()
                for piece in pieces:
                    multiply(piece, source)

            if number >= 1:

                @pl.when(t == 2 * (jnp.maximum(a, 1) - 1))
                def _():
                    chain(number - 1)

            @pl.when(t == 1)
            def _():
                for piece in pieces:
                    if piece not in peer_first:
                        arrive(piece, peer)
                    multiply(piece, peer)

            @pl.when(t >= 2)
            def _():
                from_peer(pieces, t - 2)

        if number + 1 < len(phases):
            send_mine(phases[number + 1])

        @pl.loop(steps - 2, steps)
        def _(t):
            from_peer(pieces, t)

        if number == 0:
            decays()
            local_state(0)
        elif number == 1:
            local_state(1)
            chain_end(0)
            attention(0)

    for i in range(blocks):
        relay(0, i)
    chain_end(1)
    attention(1)
    out_load.wait()
    for i in range(blocks):
        settle(0, i)
    for i in range(blocks):
        relay(1, i)
    for i in range(blocks):
        settle(1, i)

    for h in range(HALVES):

        @pl.when(b == 0)
        def _():
            pair_state(h).wait_send()

        @pl.when((b == 1) & has_up)
        def _():
            line_state(h).wait_send()

        @pl.when((b == 1) & has_down)
        def _():
            back_state(h).wait_send()

        for i in range(blocks):
            for k in range(tp - 1):
                normed_copy(h, i, col, k, pair_col).wait_send()

    for pieces in phases:
        for piece in pieces:
            copy(piece, me, send_own.at[piece, 0], peer).wait_send()

            @pl.when(has_up)
            def _():
                copy(piece, me, send_own.at[piece, 1], peer).wait_send()

            @pl.when(has_down)
            def _():
                copy(piece, me, send_own.at[piece, 2], peer).wait_send()

            if piece in peer_first:

                @pl.when(has_up)
                def _():
                    copy(piece, peer, send_line.at[piece, peer], peer).wait_send()

                @pl.when(has_down)
                def _():
                    copy(piece, peer, send_peer.at[piece, peer], peer).wait_send()

        @pl.loop(0, steps)
        def _(t):
            origin, valid, onward, target = step_of(t)
            source = origin * cross + b
            other = origin * cross + (1 - b)
            for piece in pieces:

                @pl.when(onward)
                def _():
                    copy(piece, source, send_line.at[piece, source], peer).wait_send()
                    if piece in peer_first:
                        copy(piece, other, send_line.at[piece, other], peer).wait_send()

                if piece not in peer_first:

                    @pl.when(valid)
                    def _():
                        copy(piece, source, send_peer.at[piece, source], peer).wait_send()


def on_device(
    seq,
    tp,
    tokens,
    query_weight,
    key_weight,
    value_weight,
    gate_weight,
    decay_rate,
    norm_gain,
    out_weight,
):
    count = tokens.shape[0]
    rows, width = query_weight.shape
    heads = gate_weight.shape[1]
    half = width // HALVES
    head_size = width // heads
    wide = rows % 128 == 0
    tok = tokens if wide else tokens.reshape(count, seq, rows).transpose(1, 0, 2)
    gate_t = jnp.pad(gate_weight.T, ((0, 16 - heads), (0, 0)))
    rate = jnp.pad(decay_rate, (0, 8 - heads))[:, None]
    vmem = pl.BlockSpec(memory_space=pltpu.VMEM)
    hbm = pl.BlockSpec(memory_space=pl.ANY)
    pieces = 3 * HALVES + 1
    blocks = count // 256 if count % 256 == 0 else 1
    dma = pltpu.SemaphoreType.DMA
    deep = head_size * heads // HALVES
    out_width = out_weight.shape[1]
    return pl.pallas_call(
        functools.partial(layer_kernel, seq, tp, heads, wide),
        out_shape=jax.ShapeDtypeStruct((count, out_width), jnp.bfloat16),
        in_specs=[vmem, vmem, vmem, hbm, hbm, hbm, hbm, hbm],
        out_specs=vmem,
        scratch_shapes=[
            pltpu.VMEM((seq, 16, rows), jnp.bfloat16),
            pltpu.VMEM((3 * HALVES, seq, rows, half), jnp.bfloat16),
            pltpu.VMEM((count, 16), jnp.float32),
            pltpu.VMEM((3 * HALVES, count, half), jnp.float32),
            pltpu.VMEM(out_weight.shape, jnp.bfloat16),
            pltpu.VMEM((count, out_width), jnp.float32),
            pltpu.VMEM((count, 128), jnp.float32),
            pltpu.VMEM((8, count), jnp.float32),
            pltpu.VMEM((HALVES, deep + 8, head_size), jnp.float32),
            pltpu.VMEM((HALVES, deep + 8, head_size), jnp.float32),
            pltpu.VMEM((HALVES, deep, head_size), jnp.float32),
            pltpu.VMEM((HALVES, deep, head_size), jnp.float32),
            pltpu.VMEM((HALVES, tp, count, half), jnp.bfloat16),
            dma((pieces + 1,)),
            dma((pieces, 3)),
            dma((pieces, seq)),
            dma((pieces, seq)),
            dma((pieces, seq)),
            dma((3, HALVES)),
            dma((2, HALVES)),
            dma((HALVES, blocks, tp - 1)),
            dma((HALVES, blocks, tp)),
        ],
        compiler_params=pltpu.CompilerParams(
            collective_id=0, has_side_effects=True, vmem_limit_bytes=62 * 1024 * 1024
        ),
    )(tok, rate, norm_gain[None, :], gate_t, key_weight, value_weight, query_weight, out_weight)


def solution(mesh):
    return jax.shard_map(
        functools.partial(on_device, mesh.shape["seq"], mesh.shape["tp"]),
        mesh=mesh,
        in_specs=(
            P("seq", None),
            P("seq", "tp"),
            P("seq", "tp"),
            P("seq", "tp"),
            P("seq", "tp"),
            P("tp"),
            P("tp"),
            P(None, "tp"),
        ),
        out_specs=P("seq", "tp"),
        check_vma=False,
    )
```

```python
import functools

import jax
import jax.numpy as jnp
from jax import lax
from jax.experimental import pallas as pl
from jax.experimental.pallas import tpu as pltpu
from jax.sharding import PartitionSpec as P

HALVES = 2
MESH = pl.DeviceIdType.MESH


def layer_kernel(seq, tp, heads, wide, *refs):
    tok_in, rate_ref, gain_ref, gate_in, key_in, value_in, query_in, out_in = refs[:8]
    mixed_ref = refs[8]
    gate_buf, kvq_buf, gate_acc, acc, out_buf, out_acc, wcol, wrow = refs[9:17]
    state_mine, state_peer, state_in, state_next, normed_buf = refs[17:22]
    own_sem, send_own, send_line, send_peer, recv_sem = refs[22:27]
    state_send, state_recv, normed_send, normed_recv, tok_ref = refs[27:32]
    rows = key_in.shape[0]
    half = key_in.shape[1] // HALVES
    cross = 2
    line = seq // cross
    me = lax.axis_index("seq")
    a, b = me // cross, me % cross
    peer = a * cross + (1 - b)
    count = acc.shape[1]
    head_size = 2 * half // heads
    per_half = heads // HALVES
    block = 256 if count % 256 == 0 else count
    blocks = count // block
    col = lax.axis_index("tp")
    pair_col = col + 1 - 2 * (col % 2)
    groups = tp // 2

    def buffer(piece, source):
        if piece == 0:
            return gate_buf.at[source]
        return kvq_buf.at[piece - 1, source]

    def tok(source):
        if wide:
            return tok_ref[:, pl.ds(pl.multiple_of(source * rows, rows), rows)]
        return tok_ref[source]

    def copy(piece, source, sem, target):
        return pltpu.make_async_remote_copy(
            src_ref=buffer(piece, source),
            dst_ref=buffer(piece, source),
            send_sem=sem,
            recv_sem=recv_sem.at[piece, source],
            device_id={"seq": target},
            device_id_type=MESH,
        )

    def arrive(piece, source):
        copy(piece, source, send_own.at[piece, 0], peer).wait_recv()

    phases = [[1, 0, 2, 3], [4, 5], [6]]
    peer_first = (1,)

    loads = [pltpu.make_async_copy(gate_in, gate_buf.at[me], own_sem.at[0])]
    for index in range(3 * HALVES):
        source_ref = (key_in, value_in, query_in)[index % 3]
        at = (index // 3) * half
        loads.append(
            pltpu.make_async_copy(
                source_ref.at[:, pl.ds(at, half)], kvq_buf.at[index, me], own_sem.at[index + 1]
            )
        )
    for load in loads:
        load.start()
    tok_load = pltpu.make_async_copy(tok_in, tok_ref, own_sem.at[3 * HALVES + 2])
    tok_load.start()
    out_load = pltpu.make_async_copy(out_in, out_buf, own_sem.at[3 * HALVES + 1])
    out_load.start()

    barrier = pltpu.get_barrier_semaphore()
    has_up, has_down = a < line - 1, a > 0
    pl.semaphore_signal(barrier, inc=1, device_id={"seq": peer}, device_id_type=MESH)

    @pl.when(has_up)
    def _():
        pl.semaphore_signal(barrier, inc=1, device_id={"seq": me + cross}, device_id_type=MESH)

    @pl.when(has_down)
    def _():
        pl.semaphore_signal(barrier, inc=1, device_id={"seq": me - cross}, device_id_type=MESH)

    pl.semaphore_signal(barrier, inc=1, device_id={"tp": pair_col}, device_id_type=MESH)
    for g in range(1, groups):
        pl.semaphore_signal(
            barrier, inc=1, device_id={"tp": lax.rem(col + 2 * g, tp)}, device_id_type=MESH
        )
    pl.semaphore_wait(barrier, 1 + groups + has_up.astype(jnp.int32) + has_down.astype(jnp.int32))

    def send_across(pieces):
        for piece in pieces:
            loads[piece].wait()
            copy(piece, me, send_own.at[piece, 0], peer).start()

    def send_mine(pieces):
        for piece in pieces:

            @pl.when(has_up)
            def _():
                copy(piece, me, send_own.at[piece, 1], me + cross).start()

            @pl.when(has_down)
            def _():
                copy(piece, me, send_own.at[piece, 2], me - cross).start()

    def multiply(piece, source):
        x = tok(source)
        if piece == 0:
            gate_acc[...] += lax.dot_general(
                x, gate_buf[source], (((1,), (1,)), ((), ())), preferred_element_type=jnp.float32
            )
        else:
            acc[piece - 1] += jnp.dot(
                x, kvq_buf[piece - 1, source], preferred_element_type=jnp.float32
            )

    def step_of(t):
        d = 1 + t // 2
        sign = 1 - 2 * (t % 2)
        origin = a - sign * d
        ahead = a + sign
        valid = (origin >= 0) & (origin < line)
        onward = valid & (ahead >= 0) & (ahead < line)
        return origin, valid, onward, me + sign * cross

    def from_peer(pieces, t):
        origin, valid, _, _ = step_of(t)

        @pl.when(valid)
        def _():
            source = origin * cross + (1 - b)
            for piece in pieces:
                if piece not in peer_first:
                    arrive(piece, source)
                multiply(piece, source)

    lo_state = per_half * head_size

    def decays():
        logits = jnp.concatenate(
            [gate_acc[...], jnp.zeros((count, 128 - gate_acc.shape[1]), jnp.float32)], axis=1
        ).T[:8]
        soft = jnp.maximum(logits, 0.0) + jnp.log1p(jnp.exp(-jnp.abs(logits)))
        total = -rate_ref[...] * soft
        lane = lax.broadcasted_iota(jnp.int32, total.shape, 1)
        reach = 1
        while reach < count:
            total = total + jnp.where(lane >= reach, pltpu.roll(total, reach, 1), 0.0)
            reach *= 2
        wrow[...] = total
        wcol[...] = jnp.concatenate(
            [total, jnp.zeros((120, count), jnp.float32)], axis=0
        ).T

    def state_copy(ref_from, ref_to, h, send, recv, target):
        return pltpu.make_async_remote_copy(
            src_ref=ref_from.at[h],
            dst_ref=ref_to.at[h],
            send_sem=state_send.at[send, h],
            recv_sem=state_recv.at[recv, h],
            device_id={"seq": target},
            device_id_type=MESH,
        )

    def pair_state(h):
        return state_copy(state_mine, state_peer, h, 0, 0, peer)

    def line_state(h):
        return state_copy(state_next, state_in, h, 1, 1, me + cross)

    def back_state(h):
        return state_copy(state_in, state_in, h, 2, 1, peer)

    def local_state(h):
        for j in range(per_half):
            head = h * per_half + j
            cols = slice(j * head_size, (j + 1) * head_size)
            within = wcol[:, head : head + 1]
            last = wcol[count - 1 : count, head : head + 1]
            key = acc[3 * h, :, cols].astype(jnp.bfloat16).astype(jnp.float32)
            scaled = (jnp.exp(last - within) * key).astype(jnp.bfloat16)
            value = acc[3 * h + 1, :, cols].astype(jnp.bfloat16)
            state_mine[h, j * head_size : (j + 1) * head_size] = lax.dot_general(
                scaled, value, (((0,), (0,)), ((), ())), preferred_element_type=jnp.float32
            )
            state_mine[h, lo_state + j : lo_state + j + 1] = jnp.broadcast_to(last, (1, head_size))

        @pl.when(b == 0)
        def _():
            pair_state(h).start()

        @pl.when(a == 0)
        def _():
            state_in[h] = jnp.zeros(state_in.shape[1:], jnp.float32)

    def chain(h):
        @pl.when(b == 1)
        def _():
            pair_state(h).wait_recv()

            @pl.when(has_down)
            def _():
                line_state(h).wait_recv()
                back_state(h).start()

            for j in range(per_half):
                at = slice(j * head_size, (j + 1) * head_size)
                tot = slice(lo_state + j, lo_state + j + 1)
                before = jnp.exp(state_peer[h, tot]) * state_in[h, at] + state_peer[h, at]
                state_peer[h, at] = before
                state_next[h, at] = jnp.exp(state_mine[h, tot]) * before + state_mine[h, at]

            @pl.when(has_up)
            def _():
                line_state(h).start()

    def chain_end(h):
        @pl.when(b == 0)
        def _():
            @pl.when(has_down)
            def _():
                back_state(h).wait_recv()

            state_peer[h, :lo_state] = state_in[h]

    def normed_copy(h, i, source, send, target):
        at = pl.ds(i * block, block)
        return pltpu.make_async_remote_copy(
            src_ref=normed_buf.at[h, source, at],
            dst_ref=normed_buf.at[h, source, at],
            send_sem=normed_send.at[h, i, send],
            recv_sem=normed_recv.at[h, i, source],
            device_id={"tp": target},
            device_id_type=MESH,
        )

    def far(g):
        return lax.rem(col + 2 * g, tp)

    def far_pair(g):
        return lax.rem(pair_col + 2 * g, tp)

    def attention(h, which):
        for i in which:
            t_at = slice(i * block, (i + 1) * block)
            upto = (i + 1) * block
            row = i * block + lax.broadcasted_iota(jnp.int32, (block, upto), 0)
            causal = lax.broadcasted_iota(jnp.int32, (block, upto), 1) <= row
            for j in range(per_half):
                head = h * per_half + j
                cols = slice(j * head_size, (j + 1) * head_size)
                query = acc[3 * h + 2, t_at, cols].astype(jnp.bfloat16)
                key = acc[3 * h, :upto, cols].astype(jnp.bfloat16)
                value = acc[3 * h + 1, :upto, cols].astype(jnp.bfloat16)
                within = wcol[t_at, head : head + 1]
                scores = lax.dot_general(
                    query, key, (((1,), (1,)), ((), ())), preferred_element_type=jnp.float32
                )
                gap = within - wrow[head : head + 1, :upto]
                attn = jnp.where(causal, scores * jnp.exp(jnp.where(causal, gap, 0.0)), 0.0)
                local = jnp.dot(
                    attn.astype(jnp.bfloat16), value, preferred_element_type=jnp.float32
                )
                scaled = (jnp.exp(within) * query.astype(jnp.float32)).astype(jnp.bfloat16)
                state = state_peer[h, j * head_size : (j + 1) * head_size].astype(jnp.bfloat16)
                head_out = local + jnp.dot(scaled, state, preferred_element_type=jnp.float32)
                square = jnp.mean(head_out * head_out, axis=-1, keepdims=True)
                gain = gain_ref[:, head * head_size : (head + 1) * head_size]
                normed_buf[h, col, t_at, cols] = (
                    head_out * lax.rsqrt(square + 1e-05) * gain
                ).astype(jnp.bfloat16)
            for g in range(1, groups):
                normed_copy(h, i, col, g, far(g)).start()
            normed_copy(h, i, col, 0, pair_col).start()

    def relay(h, i):
        for g in range(1, groups):
            normed_copy(h, i, far(g), 0, pair_col).wait_recv()
            normed_copy(h, i, far(g), groups - 1 + g, pair_col).start()

    def mix(h, i, source):
        at = pl.ds(i * block, block)
        depth = pl.ds(pl.multiple_of((source * HALVES + h) * half, half), half)
        return jnp.dot(
            normed_buf[h, source, at], out_buf[depth, :], preferred_element_type=jnp.float32
        )

    def settle(h, i):
        at = pl.ds(i * block, block)
        total = mix(h, i, col)
        normed_copy(h, i, pair_col, 0, pair_col).wait_recv()
        total = total + mix(h, i, pair_col)
        for g in range(1, groups):
            total = total + mix(h, i, far(g))
            normed_copy(h, i, far_pair(g), 0, pair_col).wait_recv()
            total = total + mix(h, i, far_pair(g))
        if h == 0:
            out_acc[at, :] = total
        else:
            mixed_ref[at, :] = (out_acc[at, :] + total).astype(jnp.bfloat16)

    gate_acc[...] = jnp.zeros_like(gate_acc)
    acc[...] = jnp.zeros_like(acc)
    steps = 2 * (line - 1)
    for number, pieces in enumerate(phases):
        if number == 0:
            for piece in pieces:
                send_across([piece])
                send_mine([piece])
            for later in phases[1:]:
                send_across(later)
            tok_load.wait()
        for piece in pieces:
            if piece in peer_first:
                arrive(piece, peer)

                @pl.when(has_up)
                def _():
                    copy(piece, peer, send_line.at[piece, peer], me + cross).start()

                @pl.when(has_down)
                def _():
                    copy(piece, peer, send_peer.at[piece, peer], me - cross).start()

        for piece in pieces:
            multiply(piece, me)

        @pl.loop(0, steps)
        def _(t):
            origin, valid, onward, target = step_of(t)
            source = origin * cross + b
            other = origin * cross + (1 - b)

            @pl.when(valid)
            def _():
                for piece in pieces:
                    arrive(piece, source)

                    @pl.when(onward)
                    def _():
                        copy(piece, source, send_line.at[piece, source], target).start()

                    if piece not in peer_first:
                        copy(piece, source, send_peer.at[piece, source], peer).start()
                for piece in pieces:
                    if piece in peer_first:
                        arrive(piece, other)

                        @pl.when(onward)
                        def _():
                            copy(piece, other, send_line.at[piece, other], target).start()
                for piece in pieces:
                    multiply(piece, source)

            if number >= 1:

                @pl.when(t == 2 * (jnp.maximum(a, 1) - 1))
                def _():
                    chain(number - 1)

            if number == 2:
                for i in range(blocks):

                    @pl.when(t == 2 * i + 1)
                    def _():
                        attention(0, [i])

            @pl.when(t == 1)
            def _():
                for piece in pieces:
                    if piece not in peer_first:
                        arrive(piece, peer)
                    multiply(piece, peer)

            @pl.when(t >= 2)
            def _():
                from_peer(pieces, t - 2)

        if number + 1 < len(phases):
            send_mine(phases[number + 1])

        if number == 2:
            attention(0, [i for i in range(blocks) if 2 * i + 1 >= steps])

        @pl.loop(steps - 2, steps)
        def _(t):
            from_peer(pieces, t)

        if number == 0:
            decays()
            local_state(0)
        elif number == 1:
            local_state(1)
            chain_end(0)

    for i in range(blocks):
        relay(0, i)
    chain_end(1)
    attention(1, range(blocks))
    out_load.wait()
    for i in range(blocks):
        settle(0, i)
    for i in range(blocks):
        relay(1, i)
    for i in range(blocks):
        settle(1, i)

    for h in range(HALVES):

        @pl.when(b == 0)
        def _():
            pair_state(h).wait_send()

        @pl.when((b == 1) & has_up)
        def _():
            line_state(h).wait_send()

        @pl.when((b == 1) & has_down)
        def _():
            back_state(h).wait_send()

        for i in range(blocks):
            for k in range(tp - 1):
                normed_copy(h, i, col, k, pair_col).wait_send()

    for pieces in phases:
        for piece in pieces:
            copy(piece, me, send_own.at[piece, 0], peer).wait_send()

            @pl.when(has_up)
            def _():
                copy(piece, me, send_own.at[piece, 1], peer).wait_send()

            @pl.when(has_down)
            def _():
                copy(piece, me, send_own.at[piece, 2], peer).wait_send()

            if piece in peer_first:

                @pl.when(has_up)
                def _():
                    copy(piece, peer, send_line.at[piece, peer], peer).wait_send()

                @pl.when(has_down)
                def _():
                    copy(piece, peer, send_peer.at[piece, peer], peer).wait_send()

        @pl.loop(0, steps)
        def _(t):
            origin, valid, onward, target = step_of(t)
            source = origin * cross + b
            other = origin * cross + (1 - b)
            for piece in pieces:

                @pl.when(onward)
                def _():
                    copy(piece, source, send_line.at[piece, source], peer).wait_send()
                    if piece in peer_first:
                        copy(piece, other, send_line.at[piece, other], peer).wait_send()

                if piece not in peer_first:

                    @pl.when(valid)
                    def _():
                        copy(piece, source, send_peer.at[piece, source], peer).wait_send()


def on_device(
    seq,
    tp,
    tokens,
    query_weight,
    key_weight,
    value_weight,
    gate_weight,
    decay_rate,
    norm_gain,
    out_weight,
):
    count = tokens.shape[0]
    rows, width = query_weight.shape
    heads = gate_weight.shape[1]
    half = width // HALVES
    head_size = width // heads
    wide = rows % 128 == 0
    tok = tokens if wide else tokens.reshape(count, seq, rows).transpose(1, 0, 2)
    gate_t = jnp.pad(gate_weight.T, ((0, 16 - heads), (0, 0)))
    rate = jnp.pad(decay_rate, (0, 8 - heads))[:, None]
    vmem = pl.BlockSpec(memory_space=pltpu.VMEM)
    hbm = pl.BlockSpec(memory_space=pl.ANY)
    pieces = 3 * HALVES + 1
    blocks = count // 256 if count % 256 == 0 else 1
    dma = pltpu.SemaphoreType.DMA
    deep = head_size * heads // HALVES
    out_width = out_weight.shape[1]
    return pl.pallas_call(
        functools.partial(layer_kernel, seq, tp, heads, wide),
        out_shape=jax.ShapeDtypeStruct((count, out_width), jnp.bfloat16),
        in_specs=[hbm, vmem, vmem, hbm, hbm, hbm, hbm, hbm],
        out_specs=vmem,
        scratch_shapes=[
            pltpu.VMEM((seq, 16, rows), jnp.bfloat16),
            pltpu.VMEM((3 * HALVES, seq, rows, half), jnp.bfloat16),
            pltpu.VMEM((count, 16), jnp.float32),
            pltpu.VMEM((3 * HALVES, count, half), jnp.float32),
            pltpu.VMEM(out_weight.shape, jnp.bfloat16),
            pltpu.VMEM((count, out_width), jnp.float32),
            pltpu.VMEM((count, 128), jnp.float32),
            pltpu.VMEM((8, count), jnp.float32),
            pltpu.VMEM((HALVES, deep + 8, head_size), jnp.float32),
            pltpu.VMEM((HALVES, deep + 8, head_size), jnp.float32),
            pltpu.VMEM((HALVES, deep, head_size), jnp.float32),
            pltpu.VMEM((HALVES, deep, head_size), jnp.float32),
            pltpu.VMEM((HALVES, tp, count, half), jnp.bfloat16),
            dma((pieces + 2,)),
            dma((pieces, 3)),
            dma((pieces, seq)),
            dma((pieces, seq)),
            dma((pieces, seq)),
            dma((3, HALVES)),
            dma((2, HALVES)),
            dma((HALVES, blocks, tp - 1)),
            dma((HALVES, blocks, tp)),
            pltpu.VMEM(tok.shape, jnp.bfloat16),
        ],
        compiler_params=pltpu.CompilerParams(
            collective_id=0, has_side_effects=True, vmem_limit_bytes=62 * 1024 * 1024
        ),
    )(tok, rate, norm_gain[None, :], gate_t, key_weight, value_weight, query_weight, out_weight)


def solution(mesh):
    return jax.shard_map(
        functools.partial(on_device, mesh.shape["seq"], mesh.shape["tp"]),
        mesh=mesh,
        in_specs=(
            P("seq", None),
            P("seq", "tp"),
            P("seq", "tp"),
            P("seq", "tp"),
            P("seq", "tp"),
            P("tp"),
            P("tp"),
            P(None, "tp"),
        ),
        out_specs=P("seq", "tp"),
        check_vma=False,
    )
```

```python
import functools

import jax
import jax.numpy as jnp
from jax import lax
from jax.experimental import pallas as pl
from jax.experimental.pallas import tpu as pltpu
from jax.sharding import PartitionSpec as P

HALVES = 2
MESH = pl.DeviceIdType.MESH


def layer_kernel(seq, tp, heads, wide, *refs):
    tok_in, rate_ref, gain_ref, gate_in, key_in, value_in, query_in, out_in = refs[:8]
    mixed_ref = refs[8]
    gate_buf, kvq_buf, gate_acc, acc, out_buf, out_acc, wcol, wrow = refs[9:17]
    state_mine, state_peer, state_in, state_next, normed_buf = refs[17:22]
    own_sem, send_own, send_line, send_peer, recv_sem = refs[22:27]
    state_send, state_recv, normed_send, normed_recv, tok_ref = refs[27:32]
    rows = key_in.shape[0]
    half = key_in.shape[1] // HALVES
    cross = 2
    line = seq // cross
    me = lax.axis_index("seq")
    a, b = me // cross, me % cross
    peer = a * cross + (1 - b)
    count = acc.shape[1]
    head_size = 2 * half // heads
    per_half = heads // HALVES
    block = 256 if count % 256 == 0 else count
    blocks = count // block
    col = lax.axis_index("tp")
    pair_col = col + 1 - 2 * (col % 2)
    groups = tp // 2

    def buffer(piece, source):
        if piece == 0:
            return gate_buf.at[source]
        if piece >= 3 * HALVES:
            at = pl.ds((piece - 3 * HALVES) * (half // 2), half // 2)
            return kvq_buf.at[3 * HALVES - 1, source, :, at]
        return kvq_buf.at[piece - 1, source]

    def tok(source):
        if wide:
            return tok_ref[:, pl.ds(pl.multiple_of(source * rows, rows), rows)]
        return tok_ref[source]

    def copy(piece, source, sem, target):
        return pltpu.make_async_remote_copy(
            src_ref=buffer(piece, source),
            dst_ref=buffer(piece, source),
            send_sem=sem,
            recv_sem=recv_sem.at[piece, source],
            device_id={"seq": target},
            device_id_type=MESH,
        )

    def arrive(piece, source):
        copy(piece, source, send_own.at[piece, 0], peer).wait_recv()

    phases = [[1, 0, 2, 3], [4, 5], [6, 7]]
    peer_first = (1,)

    loads = [pltpu.make_async_copy(gate_in, gate_buf.at[me], own_sem.at[0])]
    for index in range(3 * HALVES):
        source_ref = (key_in, value_in, query_in)[index % 3]
        at = (index // 3) * half
        loads.append(
            pltpu.make_async_copy(
                source_ref.at[:, pl.ds(at, half)], kvq_buf.at[index, me], own_sem.at[index + 1]
            )
        )
    for load in loads:
        load.start()
    tok_load = pltpu.make_async_copy(tok_in, tok_ref, own_sem.at[3 * HALVES + 2])
    tok_load.start()
    out_load = pltpu.make_async_copy(out_in, out_buf, own_sem.at[3 * HALVES + 1])
    out_load.start()

    barrier = pltpu.get_barrier_semaphore()
    has_up, has_down = a < line - 1, a > 0
    pl.semaphore_signal(barrier, inc=1, device_id={"seq": peer}, device_id_type=MESH)

    @pl.when(has_up)
    def _():
        pl.semaphore_signal(barrier, inc=1, device_id={"seq": me + cross}, device_id_type=MESH)

    @pl.when(has_down)
    def _():
        pl.semaphore_signal(barrier, inc=1, device_id={"seq": me - cross}, device_id_type=MESH)

    pl.semaphore_signal(barrier, inc=1, device_id={"tp": pair_col}, device_id_type=MESH)
    for g in range(1, groups):
        pl.semaphore_signal(
            barrier, inc=1, device_id={"tp": lax.rem(col + 2 * g, tp)}, device_id_type=MESH
        )
    pl.semaphore_wait(barrier, 1 + groups + has_up.astype(jnp.int32) + has_down.astype(jnp.int32))

    def send_across(pieces):
        for piece in pieces:
            if piece <= 3 * HALVES:
                loads[piece].wait()
            copy(piece, me, send_own.at[piece, 0], peer).start()

    def send_mine(pieces):
        for piece in pieces:

            @pl.when(has_up)
            def _():
                copy(piece, me, send_own.at[piece, 1], me + cross).start()

            @pl.when(has_down)
            def _():
                copy(piece, me, send_own.at[piece, 2], me - cross).start()

    def multiply(piece, source):
        x = tok(source)
        if piece == 0:
            gate_acc[...] += lax.dot_general(
                x, gate_buf[source], (((1,), (1,)), ((), ())), preferred_element_type=jnp.float32
            )
        elif piece != 3 * HALVES:
            index = min(piece, 3 * HALVES) - 1
            acc[index] += jnp.dot(
                x, kvq_buf[index, source], preferred_element_type=jnp.float32
            )

    def step_of(t):
        d = 1 + t // 2
        sign = 1 - 2 * (t % 2)
        origin = a - sign * d
        ahead = a + sign
        valid = (origin >= 0) & (origin < line)
        onward = valid & (ahead >= 0) & (ahead < line)
        return origin, valid, onward, me + sign * cross

    def from_peer(pieces, t):
        origin, valid, _, _ = step_of(t)

        @pl.when(valid)
        def _():
            source = origin * cross + (1 - b)
            for piece in pieces:
                if piece not in peer_first:
                    arrive(piece, source)
                multiply(piece, source)

    lo_state = per_half * head_size

    def decays():
        logits = jnp.concatenate(
            [gate_acc[...], jnp.zeros((count, 128 - gate_acc.shape[1]), jnp.float32)], axis=1
        ).T[:8]
        soft = jnp.maximum(logits, 0.0) + jnp.log1p(jnp.exp(-jnp.abs(logits)))
        total = -rate_ref[...] * soft
        lane = lax.broadcasted_iota(jnp.int32, total.shape, 1)
        reach = 1
        while reach < count:
            total = total + jnp.where(lane >= reach, pltpu.roll(total, reach, 1), 0.0)
            reach *= 2
        wrow[...] = total
        wcol[...] = jnp.concatenate(
            [total, jnp.zeros((120, count), jnp.float32)], axis=0
        ).T

    def state_copy(ref_from, ref_to, h, send, recv, target):
        return pltpu.make_async_remote_copy(
            src_ref=ref_from.at[h],
            dst_ref=ref_to.at[h],
            send_sem=state_send.at[send, h],
            recv_sem=state_recv.at[recv, h],
            device_id={"seq": target},
            device_id_type=MESH,
        )

    def pair_state(h):
        return state_copy(state_mine, state_peer, h, 0, 0, peer)

    def line_state(h):
        return state_copy(state_next, state_in, h, 1, 1, me + cross)

    def back_state(h):
        return state_copy(state_in, state_in, h, 2, 1, peer)

    def local_state(h):
        for j in range(per_half):
            head = h * per_half + j
            cols = slice(j * head_size, (j + 1) * head_size)
            within = wcol[:, head : head + 1]
            last = wcol[count - 1 : count, head : head + 1]
            key = acc[3 * h, :, cols].astype(jnp.bfloat16).astype(jnp.float32)
            scaled = (jnp.exp(last - within) * key).astype(jnp.bfloat16)
            value = acc[3 * h + 1, :, cols].astype(jnp.bfloat16)
            state_mine[h, j * head_size : (j + 1) * head_size] = lax.dot_general(
                scaled, value, (((0,), (0,)), ((), ())), preferred_element_type=jnp.float32
            )
            state_mine[h, lo_state + j : lo_state + j + 1] = jnp.broadcast_to(last, (1, head_size))

        @pl.when(b == 0)
        def _():
            pair_state(h).start()

        @pl.when(a == 0)
        def _():
            state_in[h] = jnp.zeros(state_in.shape[1:], jnp.float32)

    def chain(h):
        @pl.when(b == 1)
        def _():
            pair_state(h).wait_recv()

            @pl.when(has_down)
            def _():
                line_state(h).wait_recv()
                back_state(h).start()

            for j in range(per_half):
                at = slice(j * head_size, (j + 1) * head_size)
                tot = slice(lo_state + j, lo_state + j + 1)
                before = jnp.exp(state_peer[h, tot]) * state_in[h, at] + state_peer[h, at]
                state_peer[h, at] = before
                state_next[h, at] = jnp.exp(state_mine[h, tot]) * before + state_mine[h, at]

            @pl.when(has_up)
            def _():
                line_state(h).start()

    def chain_end(h):
        @pl.when(b == 0)
        def _():
            @pl.when(has_down)
            def _():
                back_state(h).wait_recv()

            state_peer[h, :lo_state] = state_in[h]

    def normed_copy(h, i, source, send, target):
        at = pl.ds(i * block, block)
        return pltpu.make_async_remote_copy(
            src_ref=normed_buf.at[h, source, at],
            dst_ref=normed_buf.at[h, source, at],
            send_sem=normed_send.at[h, i, send],
            recv_sem=normed_recv.at[h, i, source],
            device_id={"tp": target},
            device_id_type=MESH,
        )

    def far(g):
        return lax.rem(col + 2 * g, tp)

    def far_pair(g):
        return lax.rem(pair_col + 2 * g, tp)

    def attention(h, which):
        for i in which:
            t_at = slice(i * block, (i + 1) * block)
            upto = (i + 1) * block
            row = i * block + lax.broadcasted_iota(jnp.int32, (block, upto), 0)
            causal = lax.broadcasted_iota(jnp.int32, (block, upto), 1) <= row
            for j in range(per_half):
                head = h * per_half + j
                cols = slice(j * head_size, (j + 1) * head_size)
                query = acc[3 * h + 2, t_at, cols].astype(jnp.bfloat16)
                key = acc[3 * h, :upto, cols].astype(jnp.bfloat16)
                value = acc[3 * h + 1, :upto, cols].astype(jnp.bfloat16)
                within = wcol[t_at, head : head + 1]
                scores = lax.dot_general(
                    query, key, (((1,), (1,)), ((), ())), preferred_element_type=jnp.float32
                )
                gap = within - wrow[head : head + 1, :upto]
                attn = jnp.where(causal, scores * jnp.exp(jnp.where(causal, gap, 0.0)), 0.0)
                local = jnp.dot(
                    attn.astype(jnp.bfloat16), value, preferred_element_type=jnp.float32
                )
                scaled = (jnp.exp(within) * query.astype(jnp.float32)).astype(jnp.bfloat16)
                state = state_peer[h, j * head_size : (j + 1) * head_size].astype(jnp.bfloat16)
                head_out = local + jnp.dot(scaled, state, preferred_element_type=jnp.float32)
                square = jnp.mean(head_out * head_out, axis=-1, keepdims=True)
                gain = gain_ref[:, head * head_size : (head + 1) * head_size]
                normed_buf[h, col, t_at, cols] = (
                    head_out * lax.rsqrt(square + 1e-05) * gain
                ).astype(jnp.bfloat16)
            for g in range(1, groups):
                normed_copy(h, i, col, g, far(g)).start()
            normed_copy(h, i, col, 0, pair_col).start()

    def relay(h, i):
        for g in range(1, groups):
            normed_copy(h, i, far(g), 0, pair_col).wait_recv()
            normed_copy(h, i, far(g), groups - 1 + g, pair_col).start()

    def mix(h, i, source):
        at = pl.ds(i * block, block)
        depth = pl.ds(pl.multiple_of((source * HALVES + h) * half, half), half)
        return jnp.dot(
            normed_buf[h, source, at], out_buf[depth, :], preferred_element_type=jnp.float32
        )

    def settle(h, i):
        at = pl.ds(i * block, block)
        total = mix(h, i, col)
        normed_copy(h, i, pair_col, 0, pair_col).wait_recv()
        total = total + mix(h, i, pair_col)
        for g in range(1, groups):
            total = total + mix(h, i, far(g))
            normed_copy(h, i, far_pair(g), 0, pair_col).wait_recv()
            total = total + mix(h, i, far_pair(g))
        if h == 0:
            out_acc[at, :] = total
        else:
            mixed_ref[at, :] = (out_acc[at, :] + total).astype(jnp.bfloat16)

    gate_acc[...] = jnp.zeros_like(gate_acc)
    acc[...] = jnp.zeros_like(acc)
    steps = 2 * (line - 1)
    for number, pieces in enumerate(phases):
        if number == 0:
            for piece in pieces:
                send_across([piece])
                send_mine([piece])
            for later in phases[1:]:
                send_across(later)
            tok_load.wait()
        for piece in pieces:
            if piece in peer_first:
                arrive(piece, peer)

                @pl.when(has_up)
                def _():
                    copy(piece, peer, send_line.at[piece, peer], me + cross).start()

                @pl.when(has_down)
                def _():
                    copy(piece, peer, send_peer.at[piece, peer], me - cross).start()

        for piece in pieces:
            multiply(piece, me)

        @pl.loop(1, line)
        def _(d):
            sides = [step_of(2 * (d - 1) + way) for way in (0, 1)]

            for piece in pieces:
                for origin, valid, onward, target in sides:

                    @pl.when(valid)
                    def _():
                        source = origin * cross + b
                        arrive(piece, source)

                        @pl.when(onward)
                        def _():
                            copy(piece, source, send_line.at[piece, source], target).start()

                        if piece not in peer_first:
                            copy(piece, source, send_peer.at[piece, source], peer).start()

            for piece in pieces:
                if piece in peer_first:
                    for origin, valid, onward, target in sides:

                        @pl.when(valid)
                        def _():
                            other = origin * cross + (1 - b)
                            arrive(piece, other)

                            @pl.when(onward)
                            def _():
                                copy(piece, other, send_line.at[piece, other], target).start()

            for way in (0, 1):
                origin, valid, _, _ = sides[way]

                @pl.when(valid)
                def _():
                    for piece in pieces:
                        multiply(piece, origin * cross + b)

            if number >= 1:

                @pl.when(d == jnp.maximum(a, 1))
                def _():
                    chain(number - 1)

            if number == 2:

                @pl.when(d == 1)
                def _():
                    chain_end(0)

                for i in range(blocks):

                    @pl.when(d == i + 1)
                    def _():
                        attention(0, [i])

            @pl.when(d == 1)
            def _():
                for piece in pieces:
                    if piece not in peer_first:
                        arrive(piece, peer)
                    multiply(piece, peer)

            @pl.when(d >= 2)
            def _():
                from_peer(pieces, 2 * (d - 2))
                from_peer(pieces, 2 * (d - 2) + 1)

        if number + 1 < len(phases):
            send_mine(phases[number + 1])

        if number == 2:
            attention(0, range(line - 1, blocks))

        @pl.loop(steps - 2, steps)
        def _(t):
            from_peer(pieces, t)

        if number == 0:
            decays()
            local_state(0)
        elif number == 1:
            local_state(1)

    for i in range(blocks):
        relay(0, i)
    chain_end(1)
    attention(1, range(blocks))
    out_load.wait()
    for i in range(blocks):
        settle(0, i)
    for i in range(blocks):
        relay(1, i)
    for i in range(blocks):
        settle(1, i)

    for h in range(HALVES):

        @pl.when(b == 0)
        def _():
            pair_state(h).wait_send()

        @pl.when((b == 1) & has_up)
        def _():
            line_state(h).wait_send()

        @pl.when((b == 1) & has_down)
        def _():
            back_state(h).wait_send()

        for i in range(blocks):
            for k in range(tp - 1):
                normed_copy(h, i, col, k, pair_col).wait_send()

    for pieces in phases:
        for piece in pieces:
            copy(piece, me, send_own.at[piece, 0], peer).wait_send()

            @pl.when(has_up)
            def _():
                copy(piece, me, send_own.at[piece, 1], peer).wait_send()

            @pl.when(has_down)
            def _():
                copy(piece, me, send_own.at[piece, 2], peer).wait_send()

            if piece in peer_first:

                @pl.when(has_up)
                def _():
                    copy(piece, peer, send_line.at[piece, peer], peer).wait_send()

                @pl.when(has_down)
                def _():
                    copy(piece, peer, send_peer.at[piece, peer], peer).wait_send()

        @pl.loop(0, steps)
        def _(t):
            origin, valid, onward, target = step_of(t)
            source = origin * cross + b
            other = origin * cross + (1 - b)
            for piece in pieces:

                @pl.when(onward)
                def _():
                    copy(piece, source, send_line.at[piece, source], peer).wait_send()
                    if piece in peer_first:
                        copy(piece, other, send_line.at[piece, other], peer).wait_send()

                if piece not in peer_first:

                    @pl.when(valid)
                    def _():
                        copy(piece, source, send_peer.at[piece, source], peer).wait_send()


def on_device(
    seq,
    tp,
    tokens,
    query_weight,
    key_weight,
    value_weight,
    gate_weight,
    decay_rate,
    norm_gain,
    out_weight,
):
    count = tokens.shape[0]
    rows, width = query_weight.shape
    heads = gate_weight.shape[1]
    half = width // HALVES
    head_size = width // heads
    wide = rows % 128 == 0
    tok = tokens if wide else tokens.reshape(count, seq, rows).transpose(1, 0, 2)
    gate_t = jnp.pad(gate_weight.T, ((0, 16 - heads), (0, 0)))
    rate = jnp.pad(decay_rate, (0, 8 - heads))[:, None]
    vmem = pl.BlockSpec(memory_space=pltpu.VMEM)
    hbm = pl.BlockSpec(memory_space=pl.ANY)
    pieces = 3 * HALVES + 2
    blocks = count // 256 if count % 256 == 0 else 1
    dma = pltpu.SemaphoreType.DMA
    deep = head_size * heads // HALVES
    out_width = out_weight.shape[1]
    return pl.pallas_call(
        functools.partial(layer_kernel, seq, tp, heads, wide),
        out_shape=jax.ShapeDtypeStruct((count, out_width), jnp.bfloat16),
        in_specs=[hbm, vmem, vmem, hbm, hbm, hbm, hbm, hbm],
        out_specs=vmem,
        scratch_shapes=[
            pltpu.VMEM((seq, 16, rows), jnp.bfloat16),
            pltpu.VMEM((3 * HALVES, seq, rows, half), jnp.bfloat16),
            pltpu.VMEM((count, 16), jnp.float32),
            pltpu.VMEM((3 * HALVES, count, half), jnp.float32),
            pltpu.VMEM(out_weight.shape, jnp.bfloat16),
            pltpu.VMEM((count, out_width), jnp.float32),
            pltpu.VMEM((count, 128), jnp.float32),
            pltpu.VMEM((8, count), jnp.float32),
            pltpu.VMEM((HALVES, deep + 8, head_size), jnp.float32),
            pltpu.VMEM((HALVES, deep + 8, head_size), jnp.float32),
            pltpu.VMEM((HALVES, deep, head_size), jnp.float32),
            pltpu.VMEM((HALVES, deep, head_size), jnp.float32),
            pltpu.VMEM((HALVES, tp, count, half), jnp.bfloat16),
            dma((pieces + 2,)),
            dma((pieces, 3)),
            dma((pieces, seq)),
            dma((pieces, seq)),
            dma((pieces, seq)),
            dma((3, HALVES)),
            dma((2, HALVES)),
            dma((HALVES, blocks, tp - 1)),
            dma((HALVES, blocks, tp)),
            pltpu.VMEM(tok.shape, jnp.bfloat16),
        ],
        compiler_params=pltpu.CompilerParams(
            collective_id=0, has_side_effects=True, vmem_limit_bytes=62 * 1024 * 1024
        ),
    )(tok, rate, norm_gain[None, :], gate_t, key_weight, value_weight, query_weight, out_weight)


def solution(mesh):
    return jax.shard_map(
        functools.partial(on_device, mesh.shape["seq"], mesh.shape["tp"]),
        mesh=mesh,
        in_specs=(
            P("seq", None),
            P("seq", "tp"),
            P("seq", "tp"),
            P("seq", "tp"),
            P("seq", "tp"),
            P("tp"),
            P("tp"),
            P(None, "tp"),
        ),
        out_specs=P("seq", "tp"),
        check_vma=False,
    )
```
